32 devices in a mesh: rep: 2 (over y), exp: 4 (over x, core), tp: 4 (over z).
Axes of the slice: x: 2, y: 2, z: 4, core: 2. Of those that a mesh axis runs over, the one named last changes fastest.
Arguments:
- tokens: bfloat16 [256, 6144], P(('rep', 'exp'), 'tp'), parts along dimension 0, may hold values from -6 to 6
- expert_ids: int32 [256, 2], P(('rep', 'exp')), parts along dimension 0, may hold values from 0 to 3, all different within a row; in each aligned block of 32 rows (0 to 31, 32 to 63, ...) at most 20 rows name the same one
- route_logits: float32 [256, 2], P(('rep', 'exp')), parts along dimension 0, may hold values from -6 to 6
- gate_weight: bfloat16 [6144, 32768], P(None, ('exp', 'tp')), may hold values from -0.078125 to 0.078125
- up_weight: bfloat16 [6144, 32768], P(None, ('exp', 'tp')), may hold values from -0.078125 to 0.078125
- down_weight: bfloat16 [32768, 6144], P(('exp', 'tp')), may hold values from -0.0625 to 0.0625
Outputs:
- moe_out: bfloat16 [256, 6144], P(('rep', 'exp'), 'tp'), parts along dimension 0
The draws below stay inside these ranges and needn't reach their ends.
There are 2 independent parts, one for each index of `rep`. The reference program is written for one: setup_inputs(seed, part) draws one part's arguments, and reference() takes and returns one part's arrays. A program takes and returns all parts, laid end to end along the dimension named above; an argument that names none is the same for every part. Nothing has to cross between parts.
Inputs may be any that keep to these rules, and one draw needn't show every extreme that they name: `expert_ids`: each token names two different experts. In each aligned block of 32 tokens no expert is named by more than 20 tokens, a bound that some block reaches.
All inputs are finite; a program needn't handle non-finite values.
Results may differ from the reference program's by a relative error of at most 0.019.
Values may be sent and summed in bfloat16 or wider, within the bound.
A program may use at most 128 MiB of HBM per device.

```python
import math
import jax
import jax.numpy as jnp
import numpy as np
from jax import lax

D = 6144
FF = 8192
EXPERTS = 4
TOK_EXP = 32
CAP = 20
TOKENS = 128
N_EXP = 4
N_TP = 4


def steps_of(rng, extent, cuts, low, largest):
    gain, own = 1.0, jax.random.fold_in(rng, 6)
    for dim, parts in cuts:
        draws = jnp.exp(jax.random.uniform(jax.random.fold_in(own, dim), (parts,), jnp.float32, low / len(cuts), largest / len(cuts)))
        gain = gain * jnp.repeat(draws, extent[dim] // parts).reshape([-1 if axis == dim else 1 for axis in range(len(extent))])
    return gain


def routed_block(rng, own, number, rows, count, top, bound, lean):
    order = jax.random.permutation(rng, count)
    packed, common = portions_of(count, rows * top, bound, lean, True), portions_of(count, rows * top, bound, lean, False)
    places = jnp.arange(count)

    def named(lengths, rotation):
        used = int((lengths > 0).sum())
        fixed = max(1, used // 4)
        passed = fixed + (places - fixed + rotation * (used - fixed)) % max(1, count - fixed)
        return jnp.zeros((count,), jnp.int32).at[order[jnp.where(places < fixed, places, passed)]].set(jnp.asarray(lengths, jnp.int32))

    lengths = jnp.where(number % 4 == 0, named(packed, number // 4), named(common, number - number // 4 - 1))
    mixed = jax.random.permutation(jax.random.fold_in(own, 3), count)
    source_of, taker = mixed[0:count // 2 * 2:2], mixed[1:count // 2 * 2:2]
    room = jnp.minimum(lengths[source_of] - 1, bound - lengths[taker]) // 2
    room = jnp.where((source_of == order[0]) | (taker == order[0]) | (lengths[taker] == 0), 0, jnp.maximum(room, 0))
    passed = jax.random.randint(jax.random.fold_in(own, 4), (count // 2,), 0, 1 << 20) % (room + 1)
    lengths = lengths.at[source_of].add(-passed).at[taker].add(passed)
    members = jnp.searchsorted(jnp.cumsum(lengths), jnp.arange(rows * top), side="right").astype(jnp.int32)
    listing = members.reshape(top, rows).T
    listing = listing[jax.random.permutation(jax.random.fold_in(own, 1), rows)]
    rotation = jax.random.randint(jax.random.fold_in(own, 2), (rows, 1), 0, top)
    return jnp.take_along_axis(listing, (jnp.arange(top)[None, :] + rotation) % top, axis=1)


def portions_of(number_of, total, reach, skew, full):
    portions = [(1 << 20) // math.isqrt(rank ** skew) + 1 for rank in range(1, number_of + 1)]
    largest = reach if full else min(reach, max(-(-total // number_of), total * portions[0] // sum(portions)))
    least = 1 if total - largest >= number_of - 1 else 0
    counts, spare = [largest] + [least] * (number_of - 1), total - largest - least * (number_of - 1)
    while spare > 0:
        candidates = [i for i in range(1, number_of) if counts[i] < largest] or [i for i in range(1, number_of) if counts[i] < reach]
        pool, remaining = sum([portions[i] for i in candidates]), spare
        for i in candidates:
            more = min(reach - counts[i], max(1, remaining * portions[i] // pool), spare)
            counts[i] = counts[i] + more
            spare = spare - more
    return np.array(counts)


def normal_values(rng, dims, scale, reach, split=(), kind=jnp.bfloat16):
    array = scale * jax.random.normal(rng, dims, jnp.float32)
    if split:
        array = array * steps_of(rng, dims, split, -0.22, 0.18)
    return jnp.clip(array, -reach, reach).astype(kind)


def setup_inputs(seed: int = 0, part: int = 0) -> dict:
    splits = jax.random.split(jax.random.key(seed), 7)
    own_keys = jax.random.split(jax.random.fold_in(splits[6], part), 7)
    tokens = normal_values(own_keys[0], (TOKENS, D), 1.0, 6.0, ((0, 4), (1, 4)))
    expert_ids_keys = jax.random.split(jax.random.fold_in(own_keys[1], 1), TOKENS // TOK_EXP)
    expert_ids_turns = jax.random.permutation(jax.random.fold_in(own_keys[1], 3), TOKENS // TOK_EXP)
    expert_ids = jax.vmap(lambda own, number: routed_block(jax.random.fold_in(own_keys[1], 2), own, number, TOK_EXP, EXPERTS, 2, CAP, 2))(expert_ids_keys, expert_ids_turns).reshape((TOKENS, 2))
    route_logits = normal_values(own_keys[2], (TOKENS, 2), 1.5, 6.0, ((0, 4),), jnp.float32)
    gate_weight = normal_values(splits[3], (D, EXPERTS * FF), D ** -0.5, 0.078125, ((1, 16),))
    up_weight = normal_values(splits[4], (D, EXPERTS * FF), D ** -0.5, 0.078125, ((1, 16),))
    down_weight = normal_values(splits[5], (EXPERTS * FF, D), FF ** -0.5, 0.0625, ((0, 16),))
    return {"tokens": tokens, "expert_ids": expert_ids, "route_logits": route_logits, "gate_weight": gate_weight, "up_weight": up_weight, "down_weight": down_weight}


def slot_tables(expert_ids, route_logits):
    chosen = (expert_ids[:, :, None] == jnp.arange(EXPERTS, dtype=jnp.int32)[None, None, :]).astype(jnp.int32)
    per_token = jnp.sum(chosen, axis=1)
    before = jnp.cumsum(per_token, axis=0) - per_token
    position = jnp.sum(chosen * before[:, None, :], axis=2)
    at_slot = (position[:, :, None] == jnp.arange(CAP, dtype=jnp.int32)[None, None, :]).astype(jnp.float32)
    chosen_f = chosen.astype(jnp.float32)
    diff = route_logits[:, 0] - route_logits[:, 1]
    shares = jnp.stack([jax.nn.sigmoid(diff), jax.nn.sigmoid(-diff)], axis=1)
    placement = jnp.einsum('tke,tkc->ect', chosen_f, at_slot)
    mixing = jnp.einsum('tk,tke,tkc->tec', shares, chosen_f, at_slot)
    return placement, mixing


def reference(tokens, expert_ids, route_logits, gate_weight, up_weight, down_weight):
    homes = tokens.reshape(N_EXP, TOK_EXP, D)
    placement, mixing = jax.vmap(slot_tables)(expert_ids.reshape(N_EXP, TOK_EXP, 2), route_logits.reshape(N_EXP, TOK_EXP, 2))
    slots = jnp.einsum('hect,htd->ehcd', placement.astype(jnp.float32), homes.astype(jnp.float32)).astype(jnp.bfloat16)
    block_width = FF // (N_EXP // EXPERTS * N_TP)
    blocks = FF // block_width
    outputs = []
    for expert in range(EXPERTS):
        slot_rows = slots[expert].reshape(N_EXP * CAP, D)
        gate_act = jnp.dot(slot_rows, gate_weight[:, expert * FF:(expert + 1) * FF], preferred_element_type=jnp.float32)
        up_act = jnp.dot(slot_rows, up_weight[:, expert * FF:(expert + 1) * FF], preferred_element_type=jnp.float32)
        hidden = (jax.nn.silu(gate_act) * up_act).astype(jnp.bfloat16)
        hidden_blocks = jnp.transpose(hidden.reshape(N_EXP * CAP, blocks, block_width), (1, 0, 2))
        down_blocks = down_weight[expert * FF:(expert + 1) * FF].reshape(blocks, block_width, D)

        def add_block(running, piece_pair):
            term = jnp.dot(piece_pair[0], piece_pair[1], preferred_element_type=jnp.float32).astype(jnp.bfloat16)
            term = lax.optimization_barrier(term)
            return running + term.astype(jnp.float32), 0

        start = jnp.zeros((N_EXP * CAP, D), jnp.float32)
        summed, unused = lax.scan(add_block, start, (hidden_blocks, down_blocks))
        outputs.append(summed.reshape(N_EXP, CAP, D))
    expert_out = jnp.stack(outputs, axis=0)
    moe_out = jnp.einsum('htec,ehcd->htd', mixing, expert_out, precision=lax.Precision.HIGHEST)
    return moe_out.reshape(TOKENS, D).astype(jnp.bfloat16)
```

```python
import functools

import jax
import jax.numpy as jnp
from jax import lax
from jax.experimental import pallas as pl
from jax.experimental.pallas import tpu as pltpu
from jax.sharding import PartitionSpec as P

EXPERTS = 4
CORES = 2
MESH = pl.DeviceIdType.MESH
F32 = jnp.float32
BF16 = jnp.bfloat16


def near_first(n):
    order = [0]
    for d in range(1, n // 2 + 1):
        for v in (d, n - d):
            if v not in order:
                order.append(v)
    return order


def tile_of(n):
    return next(t for t in (512, 384, 256, 128) if n % t == 0)


def kernel(
    n_exp,
    n_tp,
    n_w,
    tok_ref,
    ids_ref,
    log_ref,
    gate_hbm,
    up_hbm,
    down_hbm,
    out_ref,
    gate_w,
    up_w,
    down_w,
    rows,
    acc_g,
    acc_u,
    hidden,
    share,
    wcol,
    psend,
    precv,
    comb,
    xrecv,
    zsend,
    zrecv,
    gate_sem,
    up_sem,
    down_sem,
    in_z,
    in_x,
    in_p,
    share_x,
    share_p,
    out_p,
    out_x,
    out_z,
):
    n_x = n_exp // CORES
    tok, dc = tok_ref.shape
    width = acc_g.shape[1]
    half = n_x * tok
    me = lax.axis_index("exp")
    z = lax.axis_index("tp")
    x = me // CORES
    core = me % CORES
    partner = x * CORES + (1 - core)
    peers = [lax.rem(x + k, n_x) for k in range(1, n_x)]
    order = near_first(n_tp)
    out_order = order[::-1]
    mine = pl.ds(pl.multiple_of(x * tok, tok), tok)

    def remote(src, dst, sems, idx, device):
        return pltpu.make_async_remote_copy(
            src_ref=src,
            dst_ref=dst,
            send_sem=sems.at[(0,) + idx],
            recv_sem=sems.at[(1,) + idx],
            device_id=device,
            device_id_type=MESH,
        )

    def load_in(i):
        f = lax.rem(z + order[i], n_tp)
        r = pl.ds(pl.multiple_of(f * dc, dc), dc)
        s = i % n_w
        return (
            pltpu.make_async_copy(gate_hbm.at[r, :], gate_w.at[s], gate_sem.at[s]),
            pltpu.make_async_copy(up_hbm.at[r, :], up_w.at[s], up_sem.at[s]),
        )

    def load_down(i):
        f = lax.rem(z + out_order[i], n_tp)
        c = pl.ds(pl.multiple_of(f * dc, dc), dc)
        s = i % n_w
        return pltpu.make_async_copy(down_hbm.at[:, c], down_w.at[s], down_sem.at[s])

    for i in range(n_w):
        for c in load_in(i):
            c.start()

    barrier = pltpu.get_barrier_semaphore()
    pl.semaphore_signal(barrier, inc=1, device_id={"exp": partner}, device_id_type=MESH)
    for p in peers:
        pl.semaphore_signal(
            barrier, inc=1, device_id={"exp": p * CORES + core}, device_id_type=MESH
        )
    for d in range(1, n_tp):
        pl.semaphore_signal(
            barrier, inc=1, device_id={"tp": lax.rem(z + d, n_tp)}, device_id_type=MESH
        )

    rows[0, mine, :] = tok_ref[...]
    lane = lax.broadcasted_iota(jnp.int32, (tok, 128), 1)
    diff = log_ref[:, 0:1] - log_ref[:, 1:2]
    share[0, x] = jnp.where(ids_ref[:, 0:1] == lane, jax.nn.sigmoid(diff), 0.0) + jnp.where(
        ids_ref[:, 1:2] == lane, jax.nn.sigmoid(-diff), 0.0
    )
    pl.semaphore_wait(barrier, 1 + (n_x - 1) + (n_tp - 1))

    sends = []

    def send(copy):
        copy.start()
        sends.append(copy)
        return copy

    z_in = [None] + [
        send(
            remote(
                tok_ref,
                rows.at[i, mine, :],
                in_z,
                (i,),
                {"tp": lax.rem(z + n_tp - order[i], n_tp)},
            )
        )
        for i in range(1, n_tp)
    ]
    x_in = {}

    def send_x(i):
        if i >= n_tp:
            return
        if i > 0:
            z_in[i].wait_recv()
        src = tok_ref if i == 0 else rows.at[i, mine, :]
        x_in[i] = [
            send(
                remote(
                    src, rows.at[i, mine, :], in_x, (i, k), {"exp": p * CORES + core}
                )
            )
            for k, p in enumerate(peers)
        ]

    send_x(0)
    send_x(1)
    tn = tile_of(width)
    share_in = None
    for i in range(n_tp):
        for c in x_in[i]:
            c.wait_recv()
        relay = send(
            remote(
                rows.at[i, pl.ds(0, half), :],
                rows.at[i, pl.ds(half, half), :],
                in_p,
                (i,),
                {"exp": partner},
            )
        )
        send_x(i + 2)
        if i == n_tp - 1:
            share_in = [
                send(
                    remote(
                        share.at[0, x], share.at[0, x], share_x, (k,), {"exp": p * CORES + core}
                    )
                )
                for k, p in enumerate(peers)
            ]
        relay.wait_recv()
        for c in load_in(i):
            c.wait()
        s = i % n_w

        @pl.loop(0, width // tn)
        def _(t, i=i, s=s):
            cols = pl.ds(pl.multiple_of(t * tn, tn), tn)
            a = rows[i]
            g = jnp.dot(a, gate_w[s, :, cols], preferred_element_type=F32)
            u = jnp.dot(a, up_w[s, :, cols], preferred_element_type=F32)
            if i > 0:
                g = g + acc_g[:, cols]
                u = u + acc_u[:, cols]
            if i < n_tp - 1:
                acc_g[:, cols] = g
                acc_u[:, cols] = u
            else:
                hidden[:, cols] = (g * jax.nn.sigmoid(g) * u).astype(BF16)

        if i + n_w < n_tp:
            for c in load_in(i + n_w):
                c.start()
        if i == max(n_tp - n_w - 1, 0):
            for j in range(n_w):
                load_down(j).start()

    for c in share_in:
        c.wait_recv()
    share_relay = send(
        remote(share.at[0], share.at[1], share_p, (0,), {"exp": partner})
    )
    share_relay.wait_recv()
    groups = n_exp // EXPERTS
    expert = me // groups
    lanes = lax.broadcasted_iota(jnp.int32, (CORES * half, 128), 1)
    wall = share[...].reshape(CORES * half, 128)
    wcol[...] = jnp.broadcast_to(
        jnp.sum(jnp.where(lanes == expert, wall, 0.0), axis=1, keepdims=True), wcol.shape
    )

    to = tile_of(dc)
    to_partner = {}
    to_x = {}
    to_z = {}

    def compute(i):
        load_down(i).wait()
        s = i % n_w

        @pl.loop(0, dc // to)
        def _(t):
            cols = pl.ds(pl.multiple_of(t * to, to), to)
            p = jnp.dot(hidden[...], down_w[s, :, cols], preferred_element_type=F32)
            p = p * wcol[:, 0:1]
            comb[i, :, cols] = p[:half].astype(BF16)
            psend[i, :, cols] = p[half:].astype(BF16)

        if i + n_w < n_tp:
            load_down(i + n_w).start()
        to_partner[i] = send(
            remote(psend.at[i], precv.at[i], out_p, (i,), {"exp": partner})
        )

    def combine(i):
        to_partner[i].wait_recv()
        comb[i] = (comb[i].astype(F32) + precv[i].astype(F32)).astype(BF16)
        to_x[i] = [
            send(
                remote(
                    comb.at[i, pl.ds(pl.multiple_of(p * tok, tok), tok), :],
                    xrecv.at[i, k],
                    out_x,
                    (i, k),
                    {"exp": p * CORES + core},
                )
            )
            for k, p in enumerate(peers)
        ]

    def home(i):
        total = comb[i, mine, :].astype(F32)
        for k, c in enumerate(to_x[i]):
            c.wait_recv()
            total = total + xrecv[i, k].astype(F32)
        d = out_order[i]
        if d == 0:
            return total
        zsend[i] = total.astype(BF16)
        to_z[i] = send(
            remote(zsend.at[i], zrecv.at[i], out_z, (i,), {"tp": lax.rem(z + d, n_tp)})
        )

    own = None
    lag = 3
    for i in range(n_tp + lag):
        if i < n_tp:
            compute(i)
        if 0 <= i - 1 < n_tp:
            combine(i - 1)
        if 0 <= i - lag < n_tp:
            r = home(i - lag)
            own = r if r is not None else own
    for i in to_z:
        to_z[i].wait_recv()
        own = own + zrecv[i].astype(F32)
    out_ref[...] = own.astype(BF16)
    for c in sends:
        c.wait_send()


def on_device(tokens, expert_ids, route_logits, gate_weight, up_weight, down_weight):
    n_exp = lax.axis_size("exp")
    n_tp = lax.axis_size("tp")
    n_x = n_exp // CORES
    tok, dc = tokens.shape
    width = gate_weight.shape[1]
    n_w = min(n_tp, 3)
    total = n_exp * tok
    half = n_x * tok
    dma = pltpu.SemaphoreType.DMA
    vmem = pl.BlockSpec(memory_space=pltpu.VMEM)
    hbm = pl.BlockSpec(memory_space=pl.ANY)
    return pl.pallas_call(
        functools.partial(kernel, n_exp, n_tp, n_w),
        out_shape=jax.ShapeDtypeStruct((tok, dc), BF16),
        in_specs=[vmem, vmem, vmem, hbm, hbm, hbm],
        out_specs=vmem,
        scratch_shapes=[
            pltpu.VMEM((n_w, dc, width), BF16),
            pltpu.VMEM((n_w, dc, width), BF16),
            pltpu.VMEM((n_w, width, dc), BF16),
            pltpu.VMEM((n_tp, total, dc), BF16),
            pltpu.VMEM((total, width), F32),
            pltpu.VMEM((total, width), F32),
            pltpu.VMEM((total, width), BF16),
            pltpu.VMEM((CORES, n_x, tok, 128), F32),
            pltpu.VMEM((total, 128), F32),
            pltpu.VMEM((n_tp, half, dc), BF16),
            pltpu.VMEM((n_tp, half, dc), BF16),
            pltpu.VMEM((n_tp, half, dc), BF16),
            pltpu.VMEM((n_tp, n_x - 1, tok, dc), BF16),
            pltpu.VMEM((n_tp, tok, dc), BF16),
            pltpu.VMEM((n_tp, tok, dc), BF16),
            dma((n_w,)),
            dma((n_w,)),
            dma((n_w,)),
            dma((2, n_tp)),
            dma((2, n_tp, n_x - 1)),
            dma((2, n_tp)),
            dma((2, n_x - 1)),
            dma((2, 1)),
            dma((2, n_tp)),
            dma((2, n_tp, n_x - 1)),
            dma((2, n_tp)),
        ],
        compiler_params=pltpu.CompilerParams(
            collective_id=0, has_side_effects=True, vmem_limit_bytes=67043328
        ),
    )(tokens, expert_ids, route_logits, gate_weight, up_weight, down_weight)


def solution(mesh):
    return jax.shard_map(
        on_device,
        mesh=mesh,
        in_specs=(
            P(("rep", "exp"), "tp"),
            P(("rep", "exp"), None),
            P(("rep", "exp"), None),
            P(None, ("exp", "tp")),
            P(None, ("exp", "tp")),
            P(("exp", "tp"), None),
        ),
        out_specs=P(("rep", "exp"), "tp"),
        check_vma=False,
    )
```

```python
import functools

import jax
import jax.numpy as jnp
from jax import lax
from jax.experimental import pallas as pl
from jax.experimental.pallas import tpu as pltpu
from jax.sharding import PartitionSpec as P

EXPERTS = 4
CORES = 2
MESH = pl.DeviceIdType.MESH
F32 = jnp.float32
BF16 = jnp.bfloat16


def near_first(n):
    order = [0]
    for d in range(1, n // 2 + 1):
        for v in (d, n - d):
            if v not in order:
                order.append(v)
    return order


def tile_of(n):
    return next(t for t in (512, 384, 256, 128) if n % t == 0)


def kernel(
    n_exp,
    n_tp,
    n_w,
    tok_ref,
    ids_ref,
    log_ref,
    gate_hbm,
    up_hbm,
    down_hbm,
    out_ref,
    gate_w,
    up_w,
    down_w,
    rows,
    acc_g,
    acc_u,
    hidden,
    share,
    wcol,
    psend,
    precv,
    comb,
    xrecv,
    zsend,
    zrecv,
    gate_sem,
    up_sem,
    down_sem,
    in_z,
    in_x,
    in_p,
    share_x,
    share_p,
    out_p,
    out_x,
    out_z,
):
    n_x = n_exp // CORES
    tok, dc = tok_ref.shape
    width = acc_g.shape[1]
    half = n_x * tok
    me = lax.axis_index("exp")
    z = lax.axis_index("tp")
    x = me // CORES
    core = me % CORES
    partner = x * CORES + (1 - core)
    peers = [lax.rem(x + k, n_x) for k in range(1, n_x)]
    order = near_first(n_tp)
    out_order = order[::-1]
    mine = pl.ds(pl.multiple_of(x * tok, tok), tok)

    def remote(src, dst, sems, idx, device):
        return pltpu.make_async_remote_copy(
            src_ref=src,
            dst_ref=dst,
            send_sem=sems.at[(0,) + idx],
            recv_sem=sems.at[(1,) + idx],
            device_id=device,
            device_id_type=MESH,
        )

    def load_in(i):
        f = lax.rem(z + order[i], n_tp)
        r = pl.ds(pl.multiple_of(f * dc, dc), dc)
        s = i % n_w
        return (
            pltpu.make_async_copy(gate_hbm.at[r, :], gate_w.at[s], gate_sem.at[s]),
            pltpu.make_async_copy(up_hbm.at[r, :], up_w.at[s], up_sem.at[s]),
        )

    def load_down(i):
        f = lax.rem(z + out_order[i], n_tp)
        c = pl.ds(pl.multiple_of(f * dc, dc), dc)
        s = i % n_w
        return pltpu.make_async_copy(down_hbm.at[:, c], down_w.at[s], down_sem.at[s])

    for i in range(n_w):
        for c in load_in(i):
            c.start()

    barrier = pltpu.get_barrier_semaphore()
    pl.semaphore_signal(barrier, inc=1, device_id={"exp": partner}, device_id_type=MESH)
    for p in peers:
        pl.semaphore_signal(
            barrier, inc=1, device_id={"exp": p * CORES + core}, device_id_type=MESH
        )
    for d in range(1, n_tp):
        pl.semaphore_signal(
            barrier, inc=1, device_id={"tp": lax.rem(z + d, n_tp)}, device_id_type=MESH
        )

    rows[0, mine, :] = tok_ref[...]
    lane = lax.broadcasted_iota(jnp.int32, (tok, 128), 1)
    eye = lax.broadcasted_iota(jnp.int32, (tok, tok), 0) == lax.broadcasted_iota(
        jnp.int32, (tok, tok), 1
    )

    def column(row):
        spread = jnp.where(eye, jnp.broadcast_to(row, (tok, tok)), jnp.zeros_like(row))
        return jnp.sum(spread, axis=1, keepdims=True)

    diff = column(log_ref[0:1, :] - log_ref[1:2, :])
    ids = ids_ref[...].astype(F32)
    lane = lane.astype(F32)
    share[0, x] = jnp.where(column(ids[0:1]) == lane, jax.nn.sigmoid(diff), 0.0) + jnp.where(
        column(ids[1:2]) == lane, jax.nn.sigmoid(-diff), 0.0
    )
    pl.semaphore_wait(barrier, 1 + (n_x - 1) + (n_tp - 1))

    sends = []

    def send(copy):
        copy.start()
        sends.append(copy)
        return copy

    z_in = [None] + [
        send(
            remote(
                tok_ref,
                rows.at[i, mine, :],
                in_z,
                (i,),
                {"tp": lax.rem(z + n_tp - order[i], n_tp)},
            )
        )
        for i in range(1, n_tp)
    ]
    x_in = {}

    def send_x(i):
        if i >= n_tp:
            return
        if i > 0:
            z_in[i].wait_recv()
        src = tok_ref if i == 0 else rows.at[i, mine, :]
        x_in[i] = [
            send(
                remote(
                    src, rows.at[i, mine, :], in_x, (i, k), {"exp": p * CORES + core}
                )
            )
            for k, p in enumerate(peers)
        ]

    send_x(0)
    send_x(1)
    tn = tile_of(width)
    share_in = None
    relays = {}

    def relay_rows(i):
        if i >= n_tp:
            return
        for c in x_in[i]:
            c.wait_recv()
        relays[i] = send(
            remote(
                rows.at[i, pl.ds(0, half), :],
                rows.at[i, pl.ds(half, half), :],
                in_p,
                (i,),
                {"exp": partner},
            )
        )
        send_x(i + 2)

    relay_rows(0)
    for i in range(n_tp):
        if i == n_tp - 1:
            share_in = [
                send(
                    remote(
                        share.at[0, x], share.at[0, x], share_x, (k,), {"exp": p * CORES + core}
                    )
                )
                for k, p in enumerate(peers)
            ]
        relays[i].wait_recv()
        for c in load_in(i):
            c.wait()
        s = i % n_w

        def expert_in(t, i=i, s=s):
            cols = pl.ds(pl.multiple_of(t * tn, tn), tn)
            a = rows[i]
            g = jnp.dot(a, gate_w[s, :, cols], preferred_element_type=F32)
            u = jnp.dot(a, up_w[s, :, cols], preferred_element_type=F32)
            if i > 0:
                g = g + acc_g[:, cols]
                u = u + acc_u[:, cols]
            if i < n_tp - 1:
                acc_g[:, cols] = g
                acc_u[:, cols] = u
            else:
                hidden[:, cols] = (g * jax.nn.sigmoid(g) * u).astype(BF16)

        middle = width // tn // 2
        if middle:
            pl.loop(0, middle)(expert_in)
        relay_rows(i + 1)
        pl.loop(middle, width // tn)(expert_in)

        if i + n_w < n_tp:
            for c in load_in(i + n_w):
                c.start()
        if i == max(n_tp - n_w - 1, 0):
            for j in range(n_w):
                load_down(j).start()

    for c in share_in:
        c.wait_recv()
    share_relay = send(
        remote(share.at[0], share.at[1], share_p, (0,), {"exp": partner})
    )
    share_relay.wait_recv()
    groups = n_exp // EXPERTS
    expert = me // groups
    lanes = lax.broadcasted_iota(jnp.int32, (CORES * half, 128), 1)
    wall = share[...].reshape(CORES * half, 128)
    wcol[...] = jnp.broadcast_to(
        jnp.sum(jnp.where(lanes == expert, wall, 0.0), axis=1, keepdims=True), wcol.shape
    )

    to = tile_of(dc)
    to_partner = {}
    to_x = {}
    to_z = {}

    def compute(i):
        load_down(i).wait()
        s = i % n_w

        @pl.loop(0, dc // to)
        def _(t):
            cols = pl.ds(pl.multiple_of(t * to, to), to)
            p = jnp.dot(hidden[...], down_w[s, :, cols], preferred_element_type=F32)
            p = p * wcol[:, 0:1]
            comb[i, :, cols] = p[:half].astype(BF16)
            psend[i, :, cols] = p[half:].astype(BF16)

        if i + n_w < n_tp:
            load_down(i + n_w).start()
        to_partner[i] = send(
            remote(psend.at[i], precv.at[i], out_p, (i,), {"exp": partner})
        )

    def combine(i):
        to_partner[i].wait_recv()
        comb[i] = (comb[i].astype(F32) + precv[i].astype(F32)).astype(BF16)
        to_x[i] = [
            send(
                remote(
                    comb.at[i, pl.ds(pl.multiple_of(p * tok, tok), tok), :],
                    xrecv.at[i, k],
                    out_x,
                    (i, k),
                    {"exp": p * CORES + core},
                )
            )
            for k, p in enumerate(peers)
        ]

    def home(i):
        total = comb[i, mine, :].astype(F32)
        for k, c in enumerate(to_x[i]):
            c.wait_recv()
            total = total + xrecv[i, k].astype(F32)
        d = out_order[i]
        if d == 0:
            return total
        zsend[i] = total.astype(BF16)
        to_z[i] = send(
            remote(zsend.at[i], zrecv.at[i], out_z, (i,), {"tp": lax.rem(z + d, n_tp)})
        )

    own = None
    lag = 3
    for i in range(n_tp + lag):
        if i < n_tp:
            compute(i)
        if 0 <= i - 1 < n_tp:
            combine(i - 1)
        if 0 <= i - lag < n_tp:
            r = home(i - lag)
            own = r if r is not None else own
    for i in to_z:
        to_z[i].wait_recv()
        own = own + zrecv[i].astype(F32)
    out_ref[...] = own.astype(BF16)
    for c in sends:
        c.wait_send()


def on_device(tokens, expert_ids, route_logits, gate_weight, up_weight, down_weight):
    n_exp = lax.axis_size("exp")
    n_tp = lax.axis_size("tp")
    n_x = n_exp // CORES
    tok, dc = tokens.shape
    width = gate_weight.shape[1]
    n_w = min(n_tp, 3)
    total = n_exp * tok
    half = n_x * tok
    dma = pltpu.SemaphoreType.DMA
    vmem = pl.BlockSpec(memory_space=pltpu.VMEM)
    hbm = pl.BlockSpec(memory_space=pl.ANY)
    return pl.pallas_call(
        functools.partial(kernel, n_exp, n_tp, n_w),
        out_shape=jax.ShapeDtypeStruct((tok, dc), BF16),
        in_specs=[vmem, vmem, vmem, hbm, hbm, hbm],
        out_specs=vmem,
        scratch_shapes=[
            pltpu.VMEM((n_w, dc, width), BF16),
            pltpu.VMEM((n_w, dc, width), BF16),
            pltpu.VMEM((n_w, width, dc), BF16),
            pltpu.VMEM((n_tp, total, dc), BF16),
            pltpu.VMEM((total, width), F32),
            pltpu.VMEM((total, width), F32),
            pltpu.VMEM((total, width), BF16),
            pltpu.VMEM((CORES, n_x, tok, 128), F32),
            pltpu.VMEM((total, 128), F32),
            pltpu.VMEM((n_tp, half, dc), BF16),
            pltpu.VMEM((n_tp, half, dc), BF16),
            pltpu.VMEM((n_tp, half, dc), BF16),
            pltpu.VMEM((n_tp, n_x - 1, tok, dc), BF16),
            pltpu.VMEM((n_tp, tok, dc), BF16),
            pltpu.VMEM((n_tp, tok, dc), BF16),
            dma((n_w,)),
            dma((n_w,)),
            dma((n_w,)),
            dma((2, n_tp)),
            dma((2, n_tp, n_x - 1)),
            dma((2, n_tp)),
            dma((2, n_x - 1)),
            dma((2, 1)),
            dma((2, n_tp)),
            dma((2, n_tp, n_x - 1)),
            dma((2, n_tp)),
        ],
        compiler_params=pltpu.CompilerParams(
            collective_id=0, has_side_effects=True, vmem_limit_bytes=67043328
        ),
    )(tokens, expert_ids.T, route_logits.T, gate_weight, up_weight, down_weight)


def solution(mesh):
    return jax.shard_map(
        on_device,
        mesh=mesh,
        in_specs=(
            P(("rep", "exp"), "tp"),
            P(("rep", "exp"), None),
            P(("rep", "exp"), None),
            P(None, ("exp", "tp")),
            P(None, ("exp", "tp")),
            P(("exp", "tp"), None),
        ),
        out_specs=P(("rep", "exp"), "tp"),
        check_vma=False,
    )
```
